32 devices in a mesh: ga: 2 (over core), band: 16 (over z, y, x).
Axes of the slice: x: 2, y: 2, z: 4, core: 2. Of those that a mesh axis runs over, the one named last changes fastest.
Arguments:
- orbitals: bfloat16 [1024, 2, 16384], P('band', None, 'ga'), may hold values from -6 to 6
- projectors: bfloat16 [864, 2, 16384], P(None, None, ('ga', 'band')), may hold values from -0.03125 to 0.03125
- coupling: float32 [4, 18, 18], replicated, may hold values from -6 to 6
- species: int32 [48], replicated, may hold values from 0 to 3
- offsets: int32 [48], replicated, may hold values from 0 to 846, as said below
Outputs:
- applied: bfloat16 [1024, 2, 16384], P('band', None, 'ga')
The draws below stay inside these ranges and needn't reach their ends.
Inputs may be any that keep to these rules, and one draw needn't show every extreme that they name: Each atom's 18 projectors are the 18 consecutive rows of projectors starting at its offset; offsets are multiples of 18, and the atoms' blocks are distinct and cover all 864 rows.
All inputs are finite; a program needn't handle non-finite values.
Results may differ from the reference program's by a relative error of at most 0.0049.
Values may be sent and summed in bfloat16 or wider, within the bound.
A program may use at most 64 MiB of HBM per device.

```python
import jax
import jax.numpy as jnp
from jax import lax

NBANDS = 1024
PROJ = 18
NSP = 4
ATOMS = 48
NPW = 16384
NKB = 864


def draw_offsets(key, part):
    order = jax.random.permutation(key, ATOMS)
    return (order * PROJ).astype(jnp.int32)


def plant(drawn, stream_key, smallest, largest):
    extent = drawn.shape
    spot = [jax.random.randint(jax.random.fold_in(stream_key, axis), (), 0, extent[axis]) for axis in range(len(extent))]
    drawn = drawn.at[tuple(spot)].set(smallest)
    longest = extent.index(max(extent))
    spot[longest] = (spot[longest] + 1) % extent[longest]
    return drawn.at[tuple(spot)].set(largest)


def block_scale(key, dims, cuts, least, top_value):
    gain = 1.0
    for axis_at, blocks in cuts:
        heights = jax.random.uniform(jax.random.fold_in(jax.random.fold_in(key, 6), axis_at), (blocks,), jnp.float32, least / len(cuts), top_value / len(cuts))
        gain = gain * jnp.repeat(jnp.exp(heights), dims[axis_at] // blocks).reshape((-1,) + (1,) * (len(dims) - 1 - axis_at))
    return gain


def normal_values(stream_key, shape, spread, most, pieces=(), held_as=jnp.bfloat16):
    values = spread * jax.random.normal(stream_key, shape, jnp.float32)
    if pieces:
        values = values * block_scale(stream_key, shape, pieces, -0.22, 0.18)
    return jnp.clip(values, -most, most).astype(held_as)


def setup_inputs(seed: int = 0) -> dict:
    arg_keys = jax.random.split(jax.random.key(seed), 6)
    return {
        "orbitals": normal_values(arg_keys[0], (NBANDS, 2, NPW), 1.0, 6.0, ((0, 16), (2, 2))),
        "projectors": normal_values(arg_keys[1], (NKB, 2, NPW), (2 * NPW) ** -0.5, 0.03125, ((2, 32),)),
        "coupling": normal_values(arg_keys[2], (NSP, PROJ, PROJ), ((NPW / (18 * NKB)) ** 0.5), 6.0, (), jnp.float32),
        "species": plant(jax.random.randint(arg_keys[3], (ATOMS,), 0, NSP), jax.random.fold_in(arg_keys[3], 1), 0, NSP - 1).astype(jnp.int32),
        "offsets": draw_offsets(jax.random.fold_in(arg_keys[5], 71), 0),
    }


def reference(orbitals, projectors, coupling, species, offsets):
    total_proj = projectors.shape[0]
    total_bands = orbitals.shape[0]
    per_atom = coupling.shape[1]
    flat_proj = projectors.reshape(total_proj, -1)
    turned = jnp.concatenate([orbitals[:, 1, :], -orbitals[:, 0, :]], axis=1)
    stacked = jnp.concatenate([orbitals.reshape(total_bands, -1), turned], axis=0)
    becp = lax.dot_general(flat_proj, stacked, (((1,), (1,)), ((), ())), preferred_element_type=jnp.float32)
    becp = becp.reshape(ATOMS, per_atom, 2 * total_bands)
    blocks = (offsets // per_atom).astype(jnp.int32)
    atom_kind = jnp.zeros((ATOMS,), jnp.int32).at[blocks].set(species)
    matrices = coupling[atom_kind].astype(jnp.float32)
    dbecp = jnp.einsum("aij,ajc->aic", matrices, becp, precision=lax.Precision.HIGHEST)
    dbecp = dbecp.reshape(total_proj, 2 * total_bands).astype(jnp.bfloat16)
    real_part = lax.dot_general(dbecp, projectors[:, 0, :], (((0,), (0,)), ((), ())), preferred_element_type=jnp.float32)
    imag_part = lax.dot_general(dbecp, projectors[:, 1, :], (((0,), (0,)), ((), ())), preferred_element_type=jnp.float32)
    out_real = real_part[:total_bands] - imag_part[total_bands:]
    out_imag = imag_part[:total_bands] + real_part[total_bands:]
    return jnp.stack([out_real, out_imag], axis=1).astype(jnp.bfloat16)
```

```python
import functools

import jax
import jax.numpy as jnp
from jax import lax
from jax.experimental import pallas as pl
from jax.experimental.pallas import tpu as pltpu
from jax.sharding import PartitionSpec as P

MESH = pl.DeviceIdType.MESH
INNER = 4
F32 = jnp.float32
BF16 = jnp.bfloat16


def coupling_matrix(coupling, species, offsets, total_proj):
    kinds, per_atom = coupling.shape[0], coupling.shape[1]
    column = jnp.arange(total_proj, dtype=jnp.int32)
    within = column % per_atom
    start = column - within
    kind = jnp.sum(
        jnp.where(offsets[:, None] == start[None, :], species[:, None], 0), axis=0
    )
    pick = (jnp.arange(kinds * per_atom, dtype=jnp.int32)[:, None] == (kind * per_atom + within)[None, :])
    table = jnp.transpose(coupling, (2, 0, 1)).reshape(per_atom, kinds * per_atom)
    rows = jnp.dot(table, pick.astype(F32), precision=lax.Precision.HIGHEST, preferred_element_type=F32)
    spread = (within[:, None] == jnp.arange(per_atom, dtype=jnp.int32)[None, :]).astype(F32)
    full = jnp.dot(spread, rows, precision=lax.Precision.HIGHEST, preferred_element_type=F32)
    return jnp.where(start[:, None] == start[None, :], full, 0.0)


def dot_t(a, b):
    return lax.dot_general(a, b, (((1,), (1,)), ((), ())), preferred_element_type=F32)


def dot(a, b):
    return lax.dot_general(a, b, (((1,), (0,)), ((), ())), preferred_element_type=F32)


def kernel(
    outer, groups, o_ref, p_ref, m_ref, out_ref,
    obuf, pbuf, acc, gsend, grecv, zsend, zrecv, dbuf, rbuf,
    o_send, o_recv, p_send, p_recv, l_sem, g_send, g_recv, z_send, z_recv,
    d_send, d_recv, f_send, f_recv, r_send, r_recv, q_sem,
):
    g = lax.axis_index("ga")
    me = lax.axis_index("band")
    o = me // INNER
    n = me % INNER
    bands = o_ref.shape[1]
    wide = p_ref.shape[2]
    span = INNER * wide
    rows = bands // groups
    other = 1 - g
    n1 = n + 1 - 2 * (n % 2)
    n2 = n + 2 - 4 * (n // 2)
    n3 = 3 - n

    def peer(d):
        return (o + d) % outer

    def at_outer(d):
        return {"band": peer(d) * INNER + n}

    side_x = {"band": o * INNER + n1}
    side_y = {"band": o * INNER + n2}
    twin = {"ga": other}

    barrier = pltpu.get_barrier_semaphore()
    partners = [at_outer(d) for d in range(1, outer)] + [side_x, side_y, twin]
    for partner in partners:
        pl.semaphore_signal(barrier, inc=1, device_id=partner, device_id_type=MESH)
    pl.semaphore_wait(barrier, len(partners))

    def remote(src, dst, send, recv, to):
        return pltpu.make_async_remote_copy(
            src_ref=src, dst_ref=dst, send_sem=send, recv_sem=recv, device_id=to, device_id_type=MESH
        )

    mine = pl.ds(pl.multiple_of(o * bands, bands), bands)
    o_copies = []
    for d in range(1, outer):
        src = o_ref.at[:, :, pl.ds(pl.multiple_of(peer(d) * span, span), span)]
        o_copies.append(remote(src, obuf.at[:, mine, :], o_send.at[d], o_recv.at[d], at_outer(d)))
    px = [remote(p_ref.at[c], pbuf.at[n, c], p_send.at[c], p_recv.at[c], side_x) for c in range(2)]
    py = [remote(p_ref.at[c], pbuf.at[n, c], p_send.at[2 + c], p_recv.at[2 + c], side_y) for c in range(2)]
    px[0].start()
    py[1].start()
    for copy in o_copies:
        copy.start()
    px[1].start()
    py[0].start()
    local_o = pltpu.make_async_copy(
        o_ref.at[:, :, pl.ds(pl.multiple_of(o * span, span), span)], obuf.at[:, mine, :], l_sem.at[0]
    )
    local_p = pltpu.make_async_copy(p_ref, pbuf.at[n], l_sem.at[1])
    local_o.start()
    local_p.start()

    px[0].wait_recv()
    fy = remote(pbuf.at[n1, 0], pbuf.at[n1, 0], p_send.at[4], p_recv.at[4], side_y)
    fy.start()
    py[1].wait_recv()
    fx = remote(pbuf.at[n2, 1], pbuf.at[n2, 1], p_send.at[5], p_recv.at[5], side_x)
    fx.start()
    local_o.wait()
    local_p.wait()
    px[1].wait_recv()
    py[0].wait_recv()
    for copy in o_copies:
        copy.wait_recv()

    def project(k, carry):
        slot = jnp.where(k == 0, n, jnp.where(k == 1, n1, jnp.where(k == 2, n2, n3)))
        cols = pl.ds(pl.multiple_of(slot * wide, wide), wide)
        o_real, o_imag = obuf[0, :, cols], obuf[1, :, cols]
        p_real, p_imag = pbuf[slot, 0], pbuf[slot, 1]
        acc[0] += dot_t(o_real, p_real) + dot_t(o_imag, p_imag)
        acc[1] += dot_t(o_imag, p_real) - dot_t(o_real, p_imag)
        return carry

    acc[...] = jnp.zeros_like(acc)
    lax.fori_loop(0, INNER - 1, project, 0)
    fy.wait_recv()
    fx.wait_recv()
    lax.fori_loop(INNER - 1, INNER, project, 0)

    def piece(position, core):
        return pl.ds(pl.multiple_of(position * bands + core * rows, rows), rows)

    order = list(range(1, outer)) + [0]
    g_copies = {}
    for d in order:
        gsend[d] = acc[:, piece(peer(d), other), :].astype(BF16)
        g_copies[d] = remote(gsend.at[d], grecv.at[d], g_send.at[d], g_recv.at[d], twin)
        g_copies[d].start()
    z_copies = {}
    for d in order:
        g_copies[d].wait_recv()
        if d:
            zsend[d] = (acc[:, piece(peer(d), g), :] + grecv[d].astype(F32)).astype(BF16)
            z_copies[d] = remote(zsend.at[d], zrecv.at[d], z_send.at[d], z_recv.at[d], at_outer(d))
            z_copies[d].start()
    total = acc[:, piece(o, g), :] + grecv[0].astype(F32)
    for d in range(1, outer):
        z_copies[d].wait_recv()
        total = total + zrecv[d].astype(F32)

    for c in range(2):
        coupled = lax.dot_general(
            total[c], m_ref[...], (((1,), (0,)), ((), ())),
            precision=lax.Precision.HIGHEST, preferred_element_type=F32,
        )
        dbuf[c, piece(o, g), :] = coupled.astype(BF16)

    own = dbuf.at[:, piece(o, g), :]
    d_copies = {}
    for d in range(1, outer):
        d_copies[d] = remote(own, own, d_send.at[d], d_recv.at[d], at_outer(d))
        d_copies[d].start()
    f_copies = [remote(own, own, f_send.at[0], f_recv.at[0], twin)]
    f_copies[0].start()
    for d in range(1, outer):
        d_copies[d].wait_recv()
        got = dbuf.at[:, piece(peer(outer - d), g), :]
        f_copies.append(remote(got, got, f_send.at[d], f_recv.at[d], twin))
        f_copies[d].start()
    for copy in f_copies:
        copy.wait_recv()

    def back(k, d):
        cols = pl.ds(pl.multiple_of((o * INNER + k) * wide, wide), wide)
        src = rbuf.at[k, :, pl.ds(pl.multiple_of(peer(d) * bands, bands), bands), :]
        if d == 0:
            return pltpu.make_async_copy(src, out_ref.at[:, :, cols], q_sem.at[k])
        return remote(src, out_ref.at[:, :, cols], r_send.at[k, d], r_recv.at[k, d], at_outer(d))

    def add_back(k, carry):
        d_real, d_imag = dbuf[0], dbuf[1]
        p_real, p_imag = pbuf[k, 0], pbuf[k, 1]
        rbuf[k, 0] = (dot(d_real, p_real) - dot(d_imag, p_imag)).astype(BF16)
        rbuf[k, 1] = (dot(d_real, p_imag) + dot(d_imag, p_real)).astype(BF16)
        for d in order:
            back(k, d).start()
        return carry

    lax.fori_loop(0, INNER, add_back, 0)

    for copy in o_copies + px + py + [fx, fy] + list(g_copies.values()) + list(z_copies.values()):
        copy.wait_send()
    for copy in list(d_copies.values()) + f_copies:
        copy.wait_send()

    def finish(k, carry):
        for d in order:
            back(k, d).wait()
        return carry

    lax.fori_loop(0, INNER, finish, 0)


def fused(outer, groups, orbitals, projectors, matrix):
    _, bands, reach = orbitals.shape
    _, total_proj, wide = projectors.shape
    rows = bands // groups
    height = outer * bands
    dma = pltpu.SemaphoreType.DMA
    hbm = pl.BlockSpec(memory_space=pl.ANY)
    flops = 16 * height * total_proj * INNER * wide
    return pl.pallas_call(
        functools.partial(kernel, outer, groups),
        out_shape=jax.ShapeDtypeStruct((2, bands, reach), BF16),
        in_specs=[hbm, hbm, pl.BlockSpec(memory_space=pltpu.VMEM)],
        out_specs=hbm,
        scratch_shapes=[
            pltpu.VMEM((2, height, INNER * wide), BF16),
            pltpu.VMEM((INNER, 2, total_proj, wide), BF16),
            pltpu.VMEM((2, height, total_proj), F32),
            pltpu.VMEM((outer, 2, rows, total_proj), BF16),
            pltpu.VMEM((outer, 2, rows, total_proj), BF16),
            pltpu.VMEM((outer, 2, rows, total_proj), BF16),
            pltpu.VMEM((outer, 2, rows, total_proj), BF16),
            pltpu.VMEM((2, height, total_proj), BF16),
            pltpu.VMEM((INNER, 2, height, wide), BF16),
            dma((outer,)), dma((outer,)), dma((6,)), dma((6,)), dma((2,)),
            dma((outer,)), dma((outer,)), dma((outer,)), dma((outer,)),
            dma((outer,)), dma((outer,)), dma((outer,)), dma((outer,)),
            dma((INNER, outer)), dma((INNER, outer)), dma((INNER,)),
        ],
        compiler_params=pltpu.CompilerParams(
            collective_id=0, has_side_effects=True, vmem_limit_bytes=56 * 1024 * 1024
        ),
        cost_estimate=pl.CostEstimate(flops=flops, bytes_accessed=4 * bands * reach, transcendentals=0),
    )(orbitals, projectors, matrix)


def per_device_kernel(outer, groups, orbitals, projectors, coupling, species, offsets):
    matrix = coupling_matrix(coupling, species, offsets, projectors.shape[0])
    result = fused(
        outer, groups, jnp.transpose(orbitals, (1, 0, 2)), jnp.transpose(projectors, (1, 0, 2)), matrix
    )
    return jnp.transpose(result, (1, 0, 2))


def per_device_plain(orbitals, projectors, coupling, species, offsets):
    total_proj = projectors.shape[0]
    p_real, p_imag = projectors[:, 0, :], projectors[:, 1, :]
    matrix = coupling_matrix(coupling, species, offsets, total_proj)
    spread = lax.all_to_all(orbitals, "band", split_axis=2, concat_axis=0, tiled=True)
    o_real, o_imag = spread[:, 0, :], spread[:, 1, :]
    partial_sum = jnp.stack(
        [dot_t(o_real, p_real) + dot_t(o_imag, p_imag), dot_t(o_imag, p_real) - dot_t(o_real, p_imag)], axis=1
    )
    becp = lax.psum_scatter(partial_sum, ("ga", "band"), scatter_dimension=0, tiled=True)
    coupled = jnp.einsum("bcp,pq->bcq", becp, matrix, precision=lax.Precision.HIGHEST).astype(BF16)
    dbecp = lax.all_gather(coupled, ("ga", "band"), axis=0, tiled=True)
    d_real, d_imag = dbecp[:, 0, :], dbecp[:, 1, :]
    result = jnp.stack(
        [dot(d_real, p_real) - dot(d_imag, p_imag), dot(d_real, p_imag) + dot(d_imag, p_real)], axis=1
    ).astype(BF16)
    return lax.all_to_all(result, "band", split_axis=0, concat_axis=2, tiled=True)


def solution(mesh):
    groups, members = mesh.shape["ga"], mesh.shape["band"]
    if groups == 2 and members % INNER == 0:
        body = functools.partial(per_device_kernel, members // INNER, groups)
    else:
        body = per_device_plain
    placed = (P("band", None, "ga"), P(None, None, ("ga", "band")), P(), P(), P())
    return jax.shard_map(body, mesh=mesh, in_specs=placed, out_specs=P("band", None, "ga"), check_vma=False)
```

```python
import functools

import jax
import jax.numpy as jnp
import numpy as np
from jax import lax
from jax.experimental import pallas as pl
from jax.experimental.pallas import tpu as pltpu
from jax.sharding import PartitionSpec as P

MESH = pl.DeviceIdType.MESH
INNER = 4
F32 = jnp.float32
BF16 = jnp.bfloat16


def coupling_rows(coupling, species, offsets, total_proj):
    kinds, per_atom = coupling.shape[0], coupling.shape[1]
    column = jnp.arange(total_proj, dtype=jnp.int32)
    within = column % per_atom
    start = column - within
    kind = jnp.sum(
        jnp.where(offsets[:, None] == start[None, :], species[:, None], 0), axis=0
    )
    pick = (jnp.arange(kinds * per_atom, dtype=jnp.int32)[:, None] == (kind * per_atom + within)[None, :])
    table = jnp.transpose(coupling, (2, 0, 1)).reshape(per_atom, kinds * per_atom)
    return jnp.dot(table, pick.astype(F32), precision=lax.Precision.HIGHEST, preferred_element_type=F32)


def block_diagonal(rows, spread, start_col, start_row):
    full = lax.dot_general(
        spread, rows, (((1,), (0,)), ((), ())), precision=lax.Precision.HIGHEST, preferred_element_type=F32
    )
    return jnp.where(start_col == start_row, full, 0.0)


def block_maps(count, per_atom):
    index = np.arange(count)
    spread = (index[:, None] % per_atom == np.arange(per_atom)[None, :]).astype(np.float32)
    start = (index // per_atom).astype(np.int32)
    return spread, start[:, None], start[None, :]


def dot_t(a, b):
    return lax.dot_general(a, b, (((1,), (1,)), ((), ())), preferred_element_type=F32)


def dot(a, b):
    return lax.dot_general(a, b, (((1,), (0,)), ((), ())), preferred_element_type=F32)


def kernel(
    outer, groups, o_ref, p_ref, rows_ref, spread_ref, col_ref, row_ref, out_ref,
    obuf, pbuf, acc, gsend, grecv, zsend, zrecv, dbuf, rbuf, mbuf,
    o_send, o_recv, p_send, p_recv, l_sem, g_send, g_recv, z_send, z_recv,
    d_send, d_recv, f_send, f_recv, r_send, r_recv, q_sem,
):
    parts = p_ref.shape[1]
    g = lax.axis_index("ga")
    me = lax.axis_index("band")
    o = me // INNER
    n = me % INNER
    bands = o_ref.shape[1]
    wide = p_ref.shape[3]
    span = INNER * wide
    rows = bands // groups
    other = 1 - g
    n1 = n + 1 - 2 * (n % 2)
    n2 = n + 2 - 4 * (n // 2)
    n3 = 3 - n

    def peer(d):
        return (o + d) % outer

    def at_outer(d):
        return {"band": peer(d) * INNER + n}

    side_x = {"band": o * INNER + n1}
    side_y = {"band": o * INNER + n2}
    twin = {"ga": other}

    barrier = pltpu.get_barrier_semaphore()
    partners = [at_outer(d) for d in range(1, outer)] + [side_x, side_y, twin]
    for partner in partners:
        pl.semaphore_signal(barrier, inc=1, device_id=partner, device_id_type=MESH)
    pl.semaphore_wait(barrier, len(partners))

    def remote(src, dst, send, recv, to):
        return pltpu.make_async_remote_copy(
            src_ref=src, dst_ref=dst, send_sem=send, recv_sem=recv, device_id=to, device_id_type=MESH
        )

    mine = pl.ds(pl.multiple_of(o * bands, bands), bands)
    o_copies = []
    for d in range(1, outer):
        src = o_ref.at[:, :, pl.ds(pl.multiple_of(peer(d) * span, span), span)]
        o_copies.append(remote(src, obuf.at[:, mine, :], o_send.at[d], o_recv.at[d], at_outer(d)))
    px, py, fx, fy = {}, {}, {}, {}

    def p_remote(src, slot, c, h, index, to):
        return remote(src, pbuf.at[slot, h, c], p_send.at[h, index], p_recv.at[h, index], to)

    def send_own(h):
        for c in range(2):
            px[h, c] = p_remote(p_ref.at[c, h], n, c, h, c, side_x)
            py[h, c] = p_remote(p_ref.at[c, h], n, c, h, 2 + c, side_y)
        for copy in (px[h, 0], py[h, 1], px[h, 1], py[h, 0]):
            copy.start()

    send_own(0)
    for copy in o_copies:
        copy.start()
    local = [
        pltpu.make_async_copy(
            o_ref.at[:, :, pl.ds(pl.multiple_of(o * span, span), span)], obuf.at[:, mine, :], l_sem.at[0, 0]
        )
    ]
    for h in range(parts):
        for c in range(2):
            local.append(pltpu.make_async_copy(p_ref.at[c, h], pbuf.at[n, h, c], l_sem.at[1 + h, c]))
    for copy in local:
        copy.start()

    for h in range(parts):
        px[h, 0].wait_recv()
        fy[h] = p_remote(pbuf.at[n1, h, 0], n1, 0, h, 4, side_y)
        fy[h].start()
        py[h, 1].wait_recv()
        fx[h] = p_remote(pbuf.at[n2, h, 1], n2, 1, h, 5, side_x)
        fx[h].start()
        if h < parts - 1:
            send_own(h + 1)
        mbuf[h] = block_diagonal(rows_ref[h], spread_ref[...], col_ref[...], row_ref[...])

    for copy in local:
        copy.wait()
    for copy in o_copies:
        copy.wait_recv()

    def project(h):
        def step(slot, carry):
            cols = pl.ds(pl.multiple_of(slot * wide, wide), wide)
            o_real, o_imag = obuf[0, :, cols], obuf[1, :, cols]
            p_real, p_imag = pbuf[slot, h, 0], pbuf[slot, h, 1]
            acc[h, 0] += dot_t(o_real, p_real) + dot_t(o_imag, p_imag)
            acc[h, 1] += dot_t(o_imag, p_real) - dot_t(o_real, p_imag)
            return carry

        px[h, 1].wait_recv()
        py[h, 0].wait_recv()
        fy[h].wait_recv()
        fx[h].wait_recv()
        acc[h] = jnp.zeros_like(acc[h])
        lax.fori_loop(0, INNER, step, 0)

    def piece(position, core):
        return pl.ds(pl.multiple_of(position * bands + core * rows, rows), rows)

    order = list(range(1, outer)) + [0]
    g_copies, z_copies, d_copies, f_copies = {}, {}, {}, {}

    def to_twin(h):
        for d in order:
            gsend[h, d] = acc[h, :, piece(peer(d), other), :]
            g_copies[h, d] = remote(gsend.at[h, d], grecv.at[h, d], g_send.at[h, d], g_recv.at[h, d], twin)
            g_copies[h, d].start()

    def to_outer(h):
        for d in order:
            g_copies[h, d].wait_recv()
            if d:
                zsend[h, d] = (acc[h, :, piece(peer(d), g), :] + grecv[h, d]).astype(BF16)
                z_copies[h, d] = remote(
                    zsend.at[h, d], zrecv.at[h, d], z_send.at[h, d], z_recv.at[h, d], at_outer(d)
                )
                z_copies[h, d].start()

    def couple(h):
        total = acc[h, :, piece(o, g), :] + grecv[h, 0]
        for d in range(1, outer):
            z_copies[h, d].wait_recv()
            total = total + zrecv[h, d].astype(F32)
        for c in range(2):
            coupled = lax.dot_general(
                total[c], mbuf[h], (((1,), (0,)), ((), ())),
                precision=lax.Precision.HIGHEST, preferred_element_type=F32,
            )
            dbuf[h, c, piece(o, g), :] = coupled.astype(BF16)
        own = dbuf.at[h, :, piece(o, g), :]
        for d in range(1, outer):
            d_copies[h, d] = remote(own, own, d_send.at[h, d], d_recv.at[h, d], at_outer(d))
            d_copies[h, d].start()
        f_copies[h, 0] = remote(own, own, f_send.at[h, 0], f_recv.at[h, 0], twin)
        f_copies[h, 0].start()

    def hand_on(h):
        for d in range(1, outer):
            d_copies[h, d].wait_recv()
            got = dbuf.at[h, :, piece(peer(outer - d), g), :]
            f_copies[h, d] = remote(got, got, f_send.at[h, d], f_recv.at[h, d], twin)
            f_copies[h, d].start()

    for h in range(parts - 1):
        project(h)
        to_twin(h)
    for h in range(parts - 1):
        to_outer(h)
    project(parts - 1)
    to_twin(parts - 1)
    to_outer(parts - 1)
    for h in range(parts):
        couple(h)
    for h in range(parts):
        hand_on(h)
    for copy in f_copies.values():
        copy.wait_recv()

    def back(k, d):
        cols = pl.ds(pl.multiple_of((o * INNER + k) * wide, wide), wide)
        src = rbuf.at[k, :, pl.ds(pl.multiple_of(peer(d) * bands, bands), bands), :]
        if d == 0:
            return pltpu.make_async_copy(src, out_ref.at[:, :, cols], q_sem.at[k])
        return remote(src, out_ref.at[:, :, cols], r_send.at[k, d], r_recv.at[k, d], at_outer(d))

    def add_back(k, carry):
        real = imag = 0.0
        for h in range(parts):
            d_real, d_imag = dbuf[h, 0], dbuf[h, 1]
            p_real, p_imag = pbuf[k, h, 0], pbuf[k, h, 1]
            real += dot(d_real, p_real) - dot(d_imag, p_imag)
            imag += dot(d_real, p_imag) + dot(d_imag, p_real)
        rbuf[k, 0] = real.astype(BF16)
        rbuf[k, 1] = imag.astype(BF16)
        for d in order:
            back(k, d).start()
        return carry

    lax.fori_loop(0, INNER, add_back, 0)

    for copy in o_copies:
        copy.wait_send()
    for copies in (px, py, fx, fy, g_copies, z_copies, d_copies, f_copies):
        for copy in copies.values():
            copy.wait_send()

    def finish(k, carry):
        for d in order:
            back(k, d).wait()
        return carry

    lax.fori_loop(0, INNER, finish, 0)


def fused(outer, groups, parts, orbitals, projectors, rows, maps):
    _, bands, reach = orbitals.shape
    _, _, part, wide = projectors.shape
    height = outer * bands
    piece = (parts, outer, 2, bands // groups, part)
    dma = pltpu.SemaphoreType.DMA
    hbm = pl.BlockSpec(memory_space=pl.ANY)
    flops = 16 * height * parts * part * INNER * wide
    return pl.pallas_call(
        functools.partial(kernel, outer, groups),
        out_shape=jax.ShapeDtypeStruct((2, bands, reach), BF16),
        in_specs=[hbm, hbm] + [pl.BlockSpec(memory_space=pltpu.VMEM)] * 4,
        out_specs=hbm,
        scratch_shapes=[
            pltpu.VMEM((2, height, INNER * wide), BF16),
            pltpu.VMEM((INNER, parts, 2, part, wide), BF16),
            pltpu.VMEM((parts, 2, height, part), F32),
            pltpu.VMEM(piece, F32),
            pltpu.VMEM(piece, F32),
            pltpu.VMEM(piece, BF16),
            pltpu.VMEM(piece, BF16),
            pltpu.VMEM((parts, 2, height, part), BF16),
            pltpu.VMEM((INNER, 2, height, wide), BF16),
            pltpu.VMEM((parts, part, part), F32),
            dma((outer,)), dma((outer,)), dma((parts, 6)), dma((parts, 6)), dma((1 + parts, 2)),
        ] + [dma((parts, outer))] * 8 + [
            dma((INNER, outer)), dma((INNER, outer)), dma((INNER,)),
        ],
        compiler_params=pltpu.CompilerParams(
            collective_id=0, has_side_effects=True, vmem_limit_bytes=56 * 1024 * 1024
        ),
        cost_estimate=pl.CostEstimate(flops=flops, bytes_accessed=4 * bands * reach, transcendentals=0),
    )(orbitals, projectors, rows, *maps)


def count_parts(total_proj, per_atom):
    for parts in (3, 2):
        if total_proj % (parts * per_atom) == 0 and total_proj % (parts * 16) == 0:
            return parts
    return 1


def per_device_kernel(outer, groups, orbitals, projectors, coupling, species, offsets):
    total_proj, _, wide = projectors.shape
    per_atom = coupling.shape[1]
    parts = count_parts(total_proj, per_atom)
    part = total_proj // parts
    rows = coupling_rows(coupling, species, offsets, total_proj)
    rows = jnp.transpose(rows.reshape(per_atom, parts, part), (1, 0, 2))
    maps = [jnp.asarray(m) for m in block_maps(part, per_atom)]
    turned = jnp.transpose(projectors, (1, 0, 2)).reshape(2, parts, part, wide)
    result = fused(outer, groups, parts, jnp.transpose(orbitals, (1, 0, 2)), turned, rows, maps)
    return jnp.transpose(result, (1, 0, 2))


def per_device_plain(orbitals, projectors, coupling, species, offsets):
    total_proj = projectors.shape[0]
    p_real, p_imag = projectors[:, 0, :], projectors[:, 1, :]
    rows = coupling_rows(coupling, species, offsets, total_proj)
    matrix = block_diagonal(rows, *block_maps(total_proj, coupling.shape[1]))
    spread = lax.all_to_all(orbitals, "band", split_axis=2, concat_axis=0, tiled=True)
    o_real, o_imag = spread[:, 0, :], spread[:, 1, :]
    partial_sum = jnp.stack(
        [dot_t(o_real, p_real) + dot_t(o_imag, p_imag), dot_t(o_imag, p_real) - dot_t(o_real, p_imag)], axis=1
    )
    becp = lax.psum_scatter(partial_sum, ("ga", "band"), scatter_dimension=0, tiled=True)
    coupled = jnp.einsum("bcp,pq->bcq", becp, matrix, precision=lax.Precision.HIGHEST).astype(BF16)
    dbecp = lax.all_gather(coupled, ("ga", "band"), axis=0, tiled=True)
    d_real, d_imag = dbecp[:, 0, :], dbecp[:, 1, :]
    result = jnp.stack(
        [dot(d_real, p_real) - dot(d_imag, p_imag), dot(d_real, p_imag) + dot(d_imag, p_real)], axis=1
    ).astype(BF16)
    return lax.all_to_all(result, "band", split_axis=0, concat_axis=2, tiled=True)


def solution(mesh):
    groups, members = mesh.shape["ga"], mesh.shape["band"]
    if groups == 2 and members % INNER == 0:
        body = functools.partial(per_device_kernel, members // INNER, groups)
    else:
        body = per_device_plain
    placed = (P("band", None, "ga"), P(None, None, ("ga", "band")), P(), P(), P())
    return jax.shard_map(body, mesh=mesh, in_specs=placed, out_specs=P("band", None, "ga"), check_vma=False)
```

```python
import functools

import jax
import jax.numpy as jnp
import numpy as np
from jax import lax
from jax.experimental import pallas as pl
from jax.experimental.pallas import tpu as pltpu
from jax.sharding import PartitionSpec as P

MESH = pl.DeviceIdType.MESH
INNER = 4
F32 = jnp.float32
BF16 = jnp.bfloat16


def coupling_rows(coupling, species, offsets, total_proj):
    kinds, per_atom = coupling.shape[0], coupling.shape[1]
    column = jnp.arange(total_proj, dtype=jnp.int32)
    within = column % per_atom
    start = column - within
    kind = jnp.sum(
        jnp.where(offsets[:, None] == start[None, :], species[:, None], 0), axis=0
    )
    pick = (jnp.arange(kinds * per_atom, dtype=jnp.int32)[:, None] == (kind * per_atom + within)[None, :])
    table = jnp.transpose(coupling, (2, 0, 1)).reshape(per_atom, kinds * per_atom)
    return jnp.dot(table, pick.astype(F32), precision=lax.Precision.HIGHEST, preferred_element_type=F32)


def block_diagonal(rows, spread, start_col, start_row):
    full = lax.dot_general(
        spread, rows, (((1,), (0,)), ((), ())), precision=lax.Precision.HIGHEST, preferred_element_type=F32
    )
    return jnp.where(start_col == start_row, full, 0.0)


def block_maps(count, per_atom):
    index = np.arange(count)
    spread = (index[:, None] % per_atom == np.arange(per_atom)[None, :]).astype(np.float32)
    start = (index // per_atom).astype(np.int32)
    return spread, start[:, None], start[None, :]


def dot_t(a, b):
    return lax.dot_general(a, b, (((1,), (1,)), ((), ())), preferred_element_type=F32)


def dot(a, b):
    return lax.dot_general(a, b, (((1,), (0,)), ((), ())), preferred_element_type=F32)


def kernel(
    outer, groups, o_ref, p_ref, rows_ref, spread_ref, col_ref, row_ref, out_ref,
    obuf, pbuf, acc, gsend, grecv, zsend, zrecv, dbuf, rbuf, mbuf,
    o_send, o_recv, p_send, p_recv, l_sem, g_send, g_recv, z_send, z_recv,
    d_send, d_recv, f_send, f_recv, r_send, r_recv, q_sem,
):
    parts = p_ref.shape[1]
    g = lax.axis_index("ga")
    me = lax.axis_index("band")
    o = me // INNER
    n = me % INNER
    bands = o_ref.shape[1]
    wide = p_ref.shape[3]
    span = INNER * wide
    rows = bands // groups
    other = 1 - g
    n1 = n + 1 - 2 * (n % 2)
    n2 = n + 2 - 4 * (n // 2)
    n3 = 3 - n

    def peer(d):
        return (o + d) % outer

    def at_outer(d):
        return {"band": peer(d) * INNER + n}

    side_x = {"band": o * INNER + n1}
    side_y = {"band": o * INNER + n2}
    twin = {"ga": other}

    barrier = pltpu.get_barrier_semaphore()
    partners = [at_outer(d) for d in range(1, outer)] + [side_x, side_y, twin]
    for partner in partners:
        pl.semaphore_signal(barrier, inc=1, device_id=partner, device_id_type=MESH)
    pl.semaphore_wait(barrier, len(partners))

    def remote(src, dst, send, recv, to):
        return pltpu.make_async_remote_copy(
            src_ref=src, dst_ref=dst, send_sem=send, recv_sem=recv, device_id=to, device_id_type=MESH
        )

    mine = pl.ds(pl.multiple_of(o * bands, bands), bands)
    o_copies = []
    for d in range(1, outer):
        src = o_ref.at[:, :, pl.ds(pl.multiple_of(peer(d) * span, span), span)]
        o_copies.append(remote(src, obuf.at[:, mine, :], o_send.at[d], o_recv.at[d], at_outer(d)))
    px, py, fx, fy = {}, {}, {}, {}

    def p_remote(src, slot, c, h, index, to):
        return remote(src, pbuf.at[slot, h, c], p_send.at[h, index], p_recv.at[h, index], to)

    def send_own(h):
        for c in range(2):
            px[h, c] = p_remote(p_ref.at[c, h], n, c, h, c, side_x)
            py[h, c] = p_remote(p_ref.at[c, h], n, c, h, 2 + c, side_y)
        for copy in (px[h, 0], py[h, 1], px[h, 1], py[h, 0]):
            copy.start()

    send_own(0)
    for copy in o_copies:
        copy.start()
    local = [
        pltpu.make_async_copy(
            o_ref.at[:, :, pl.ds(pl.multiple_of(o * span, span), span)], obuf.at[:, mine, :], l_sem.at[0, 0]
        )
    ]
    for h in range(parts):
        for c in range(2):
            local.append(pltpu.make_async_copy(p_ref.at[c, h], pbuf.at[n, h, c], l_sem.at[1 + h, c]))
    for copy in local:
        copy.start()

    for h in range(parts):
        px[h, 0].wait_recv()
        fy[h] = p_remote(pbuf.at[n1, h, 0], n1, 0, h, 4, side_y)
        fy[h].start()
        py[h, 1].wait_recv()
        fx[h] = p_remote(pbuf.at[n2, h, 1], n2, 1, h, 5, side_x)
        fx[h].start()
        if h < parts - 1:
            send_own(h + 1)
        mbuf[h] = block_diagonal(rows_ref[h], spread_ref[...], col_ref[...], row_ref[...])

    for copy in local:
        copy.wait()
    for copy in o_copies:
        copy.wait_recv()

    def project(h):
        def step(slot, carry):
            cols = pl.ds(pl.multiple_of(slot * wide, wide), wide)
            o_real, o_imag = obuf[0, :, cols], obuf[1, :, cols]
            p_real, p_imag = pbuf[slot, h, 0], pbuf[slot, h, 1]
            acc[h, 0] += dot_t(o_real, p_real) + dot_t(o_imag, p_imag)
            acc[h, 1] += dot_t(o_imag, p_real) - dot_t(o_real, p_imag)
            return carry

        px[h, 1].wait_recv()
        py[h, 0].wait_recv()
        fy[h].wait_recv()
        fx[h].wait_recv()
        acc[h] = jnp.zeros_like(acc[h])
        lax.fori_loop(0, INNER, step, 0)

    def piece(position, core):
        return pl.ds(pl.multiple_of(position * bands + core * rows, rows), rows)

    order = list(range(1, outer)) + [0]
    g_copies, z_copies, d_copies, f_copies = {}, {}, {}, {}

    def to_twin(h):
        for d in order:
            gsend[h, d] = acc[h, :, piece(peer(d), other), :]
            g_copies[h, d] = remote(gsend.at[h, d], grecv.at[h, d], g_send.at[h, d], g_recv.at[h, d], twin)
            g_copies[h, d].start()

    def to_outer(h):
        for d in order:
            g_copies[h, d].wait_recv()
            if d:
                zsend[h, d] = (acc[h, :, piece(peer(d), g), :] + grecv[h, d]).astype(BF16)
                z_copies[h, d] = remote(
                    zsend.at[h, d], zrecv.at[h, d], z_send.at[h, d], z_recv.at[h, d], at_outer(d)
                )
                z_copies[h, d].start()

    def couple(h):
        total = acc[h, :, piece(o, g), :] + grecv[h, 0]
        for d in range(1, outer):
            z_copies[h, d].wait_recv()
            total = total + zrecv[h, d].astype(F32)
        for c in range(2):
            coupled = lax.dot_general(
                total[c], mbuf[h], (((1,), (0,)), ((), ())),
                precision=lax.Precision.HIGHEST, preferred_element_type=F32,
            )
            dbuf[h, c, piece(o, g), :] = coupled.astype(BF16)
        own = dbuf.at[h, :, piece(o, g), :]
        for d in range(1, outer):
            d_copies[h, d] = remote(own, own, d_send.at[h, d], d_recv.at[h, d], at_outer(d))
            d_copies[h, d].start()
        f_copies[h, 0] = remote(own, own, f_send.at[h, 0], f_recv.at[h, 0], twin)
        f_copies[h, 0].start()

    def hand_on(h):
        for d in range(1, outer):
            d_copies[h, d].wait_recv()
            got = dbuf.at[h, :, piece(peer(outer - d), g), :]
            f_copies[h, d] = remote(got, got, f_send.at[h, d], f_recv.at[h, d], twin)
            f_copies[h, d].start()

    for h in range(parts - 1):
        project(h)
        to_twin(h)
    for h in range(parts - 1):
        to_outer(h)
    project(parts - 1)
    to_twin(parts - 1)
    to_outer(parts - 1)
    for h in range(parts):
        couple(h)
    for h in range(parts):
        hand_on(h)
    for copy in f_copies.values():
        copy.wait_recv()

    def back(k, d):
        cols = pl.ds(pl.multiple_of((o * INNER + k) * wide, wide), wide)
        src = rbuf.at[k, :, pl.ds(pl.multiple_of(peer(d) * bands, bands), bands), :]
        if d == 0:
            return pltpu.make_async_copy(src, out_ref.at[:, :, cols], q_sem.at[k])
        return remote(src, out_ref.at[:, :, cols], r_send.at[k, d], r_recv.at[k, d], at_outer(d))

    def add_back(k, carry):
        real = imag = 0.0
        for h in range(parts):
            d_real, d_imag = dbuf[h, 0], dbuf[h, 1]
            p_real, p_imag = pbuf[k, h, 0], pbuf[k, h, 1]
            real += dot(d_real, p_real) - dot(d_imag, p_imag)
            imag += dot(d_real, p_imag) + dot(d_imag, p_real)
        rbuf[k, 0] = real.astype(BF16)
        rbuf[k, 1] = imag.astype(BF16)
        for d in order:
            back(k, d).start()
        return carry

    lax.fori_loop(0, INNER, add_back, 0)

    for copy in o_copies:
        copy.wait_send()
    for copies in (px, py, fx, fy, g_copies, z_copies, d_copies, f_copies):
        for copy in copies.values():
            copy.wait_send()

    def finish(k, carry):
        for d in order:
            back(k, d).wait()
        return carry

    lax.fori_loop(0, INNER, finish, 0)


def fused(outer, groups, parts, orbitals, projectors, rows, maps):
    _, bands, reach = orbitals.shape
    _, _, part, wide = projectors.shape
    height = outer * bands
    piece = (parts, outer, 2, bands // groups, part)
    dma = pltpu.SemaphoreType.DMA
    hbm = pl.BlockSpec(memory_space=pl.ANY)
    flops = 16 * height * parts * part * INNER * wide
    return pl.pallas_call(
        functools.partial(kernel, outer, groups),
        out_shape=jax.ShapeDtypeStruct((2, bands, reach), BF16),
        in_specs=[hbm, hbm] + [pl.BlockSpec(memory_space=pltpu.VMEM)] * 4,
        out_specs=hbm,
        scratch_shapes=[
            pltpu.VMEM((2, height, INNER * wide), BF16),
            pltpu.VMEM((INNER, parts, 2, part, wide), BF16),
            pltpu.VMEM((parts, 2, height, part), F32),
            pltpu.VMEM(piece, F32),
            pltpu.VMEM(piece, F32),
            pltpu.VMEM(piece, BF16),
            pltpu.VMEM(piece, BF16),
            pltpu.VMEM((parts, 2, height, part), BF16),
            pltpu.VMEM((INNER, 2, height, wide), BF16),
            pltpu.VMEM((parts, part, part), F32),
            dma((outer,)), dma((outer,)), dma((parts, 6)), dma((parts, 6)), dma((1 + parts, 2)),
        ] + [dma((parts, outer))] * 8 + [
            dma((INNER, outer)), dma((INNER, outer)), dma((INNER,)),
        ],
        compiler_params=pltpu.CompilerParams(
            collective_id=0, has_side_effects=True, vmem_limit_bytes=32 * 1024 * 1024
        ),
        cost_estimate=pl.CostEstimate(flops=flops, bytes_accessed=4 * bands * reach, transcendentals=0),
    )(orbitals, projectors, rows, *maps)


def count_parts(total_proj, per_atom):
    for parts in (3, 2):
        if total_proj % (parts * per_atom) == 0 and total_proj % (parts * 16) == 0:
            return parts
    return 1


def per_device_kernel(outer, groups, orbitals, projectors, coupling, species, offsets):
    total_proj, _, wide = projectors.shape
    per_atom = coupling.shape[1]
    parts = count_parts(total_proj, per_atom)
    part = total_proj // parts
    rows = coupling_rows(coupling, species, offsets, total_proj)
    rows = jnp.transpose(rows.reshape(per_atom, parts, part), (1, 0, 2))
    maps = [jnp.asarray(m) for m in block_maps(part, per_atom)]
    turned = jnp.transpose(projectors, (1, 0, 2)).reshape(2, parts, part, wide)
    result = fused(outer, groups, parts, jnp.transpose(orbitals, (1, 0, 2)), turned, rows, maps)
    return jnp.transpose(result, (1, 0, 2))


def per_device_plain(orbitals, projectors, coupling, species, offsets):
    total_proj = projectors.shape[0]
    p_real, p_imag = projectors[:, 0, :], projectors[:, 1, :]
    rows = coupling_rows(coupling, species, offsets, total_proj)
    matrix = block_diagonal(rows, *block_maps(total_proj, coupling.shape[1]))
    spread = lax.all_to_all(orbitals, "band", split_axis=2, concat_axis=0, tiled=True)
    o_real, o_imag = spread[:, 0, :], spread[:, 1, :]
    partial_sum = jnp.stack(
        [dot_t(o_real, p_real) + dot_t(o_imag, p_imag), dot_t(o_imag, p_real) - dot_t(o_real, p_imag)], axis=1
    )
    becp = lax.psum_scatter(partial_sum, ("ga", "band"), scatter_dimension=0, tiled=True)
    coupled = jnp.einsum("bcp,pq->bcq", becp, matrix, precision=lax.Precision.HIGHEST).astype(BF16)
    dbecp = lax.all_gather(coupled, ("ga", "band"), axis=0, tiled=True)
    d_real, d_imag = dbecp[:, 0, :], dbecp[:, 1, :]
    result = jnp.stack(
        [dot(d_real, p_real) - dot(d_imag, p_imag), dot(d_real, p_imag) + dot(d_imag, p_real)], axis=1
    ).astype(BF16)
    return lax.all_to_all(result, "band", split_axis=0, concat_axis=2, tiled=True)


def solution(mesh):
    groups, members = mesh.shape["ga"], mesh.shape["band"]
    if groups == 2 and members % INNER == 0:
        body = functools.partial(per_device_kernel, members // INNER, groups)
    else:
        body = per_device_plain
    placed = (P("band", None, "ga"), P(None, None, ("ga", "band")), P(), P(), P())
    return jax.shard_map(body, mesh=mesh, in_specs=placed, out_specs=P("band", None, "ga"), check_vma=False)
```
